1024 devices in a mesh: dp: 64 (over x, z), seq: 16 (over y, core).
Axes of the slice: x: 8, y: 8, z: 8, core: 2. Of those that a mesh axis runs over, the one named last changes fastest.
Arguments:
- spatial_qkv: bfloat16 [64, 3, 16, 128, 1152], P('dp', None, 'seq'), may hold values from -24 to 24
- temporal_qkv: bfloat16 [64, 3, 16, 128, 1152], P('dp', None, 'seq'), may hold values from -24 to 24
- cotangent: bfloat16 [64, 16, 128, 1152], P('dp', 'seq'), may hold values from -6 to 6
- spatial_gate: float32 [64, 1152], P('dp'), may hold values from -4 to 4
- temporal_gate: float32 [64, 1152], P('dp'), may hold values from -4 to 4
- temporal_proj: bfloat16 [1152, 1152], replicated, may hold values from -0.1875 to 0.1875
- live_counts: int32 [64, 2], P('dp'), may hold values from 2 to 128, as said below
Outputs:
- temporal_qkv_grad: bfloat16 [64, 3, 16, 128, 1152], P('dp', None, 'seq')
- spatial_proj_grad: float32 [1152, 1152], P('seq', 'dp')
- temporal_proj_grad: float32 [1152, 1152], P('seq', 'dp')
The draws below stay inside these ranges and needn't reach their ends.
Inputs may be any that keep to these rules, and one draw needn't show every extreme that they name: live_counts[g, 0] counts a clip's live frames, at most 16; live_counts[g, 1] counts the live positions of each of its frames, at most 128; in every draw some clip has all 16 frames and all 128 positions live.
All inputs are finite; a program needn't handle non-finite values.
Results may differ from the reference program's by a relative error of at most 0.015.
Values may be sent and summed in bfloat16 or wider, within the bound.
No kernel may reach another device: no remote copies, remote signals or barrier semaphores. Data moves between devices by JAX's collectives and lax.ppermute only.
A program may use at most 64 MiB of HBM per device.

```python
import jax
import jax.numpy as jnp
from jax import lax

D = 1152
HEADS = 16
FR_DEV = 1
POS = 128
HD = 72
FRAMES = 16
GROUPS = 64
N_SEQ = 16


def make_attention_inputs(base_key):
    first_key = jax.random.fold_in(base_key, 0)
    drawn = jax.random.truncated_normal(first_key, -6.0, 6.0, (GROUPS, 3, FRAMES, POS, D), jnp.float32)
    return drawn.astype(jnp.bfloat16)


def draw_spatial_qkv(key, part):
    return make_attention_inputs(jax.random.fold_in(key, 11))


def draw_temporal_qkv(key, part):
    return make_attention_inputs(jax.random.fold_in(key, 12))


def draw_live_counts(key, part):
    first_key, second_key, third_key = jax.random.split(jax.random.fold_in(key, 13), 3)
    frame_counts = jax.random.randint(first_key, (GROUPS,), max(2, FRAMES // 4), FRAMES + 1)
    position_counts = jax.random.randint(second_key, (GROUPS,), max(2, POS // 4), POS + 1)
    full_group = jax.random.randint(third_key, (), 0, GROUPS)
    group_ids = jnp.arange(GROUPS)
    frame_counts = jnp.where(group_ids == full_group, FRAMES, frame_counts)
    position_counts = jnp.where(group_ids == full_group, POS, position_counts)
    return jnp.stack([frame_counts, position_counts], axis=1).astype(jnp.int32)


def level_of(stream_key, dims, pieces, low, high):
    factor_of = 1.0
    for dim, blocks in pieces:
        steps = jax.random.uniform(jax.random.fold_in(jax.random.fold_in(stream_key, 6), dim), (blocks,), jnp.float32, low / len(pieces), high / len(pieces))
        factor_of = factor_of * jnp.repeat(jnp.exp(steps), dims[dim] // blocks).reshape((-1,) + (1,) * (len(dims) - 1 - dim))
    return factor_of


def normal_values(own_key, shape, width, most, cuts=(), kind=jnp.bfloat16):
    gain = level_of(own_key, shape, cuts, -0.22, 0.18) if cuts else 1.0
    array = jax.random.normal(own_key, shape, jnp.float32) * width * gain
    return jnp.minimum(jnp.maximum(array, -most), most).astype(kind)


def setup_inputs(seed: int = 0) -> dict:
    splits = jax.random.split(jax.random.key(seed), 8)
    spatial_qkv = draw_spatial_qkv(jax.random.fold_in(splits[7], 71), 0)
    temporal_qkv = draw_temporal_qkv(jax.random.fold_in(splits[7], 71), 0)
    cotangent = normal_values(splits[2], (GROUPS, FRAMES, POS, D), 1.0, 6.0, ((0, 64), (1, 16)))
    spatial_gate = normal_values(splits[3], (GROUPS, D), 1.0, 4.0, ((0, 64),), jnp.float32)
    temporal_gate = normal_values(splits[4], (GROUPS, D), 1.0, 4.0, ((0, 64),), jnp.float32)
    temporal_proj = normal_values(splits[5], (D, D), D ** -0.5, 0.1875)
    live_counts = draw_live_counts(jax.random.fold_in(splits[7], 71), 0)
    return {"spatial_qkv": spatial_qkv, "temporal_qkv": temporal_qkv, "cotangent": cotangent, "spatial_gate": spatial_gate, "temporal_gate": temporal_gate, "temporal_proj": temporal_proj, "live_counts": live_counts}


def attend(queries, key_block, value_block, key_keep, score_form, mix_form):
    head_split = queries.shape[:-1] + (HEADS, HD)
    q_heads = queries.astype(jnp.float32).reshape(head_split)
    k_heads = key_block.astype(jnp.float32).reshape(head_split)
    v_heads = value_block.astype(jnp.float32).reshape(head_split)
    scores = jnp.einsum(score_form, q_heads, k_heads) * HD ** (-0.5)
    scores = jnp.where(key_keep[:, None, None, :], scores, -1e+30)
    shifted = scores - lax.optimization_barrier(jnp.max(scores, axis=-1, keepdims=True))
    expo = jnp.exp(shifted)
    attention_weights = expo / lax.optimization_barrier(jnp.sum(expo, axis=-1, keepdims=True))
    rounded = lax.optimization_barrier(attention_weights.astype(jnp.bfloat16)).astype(jnp.float32)
    mixed = jnp.einsum(mix_form, rounded, v_heads)
    return mixed.reshape(queries.shape)

def block_parts(outputs, errors):
    left = outputs.reshape(N_SEQ, FR_DEV * POS, D).astype(jnp.float32)
    right = errors.reshape(N_SEQ, FR_DEV * POS, D).astype(jnp.float32)
    parts = jnp.einsum('btr,btc->brc', left, right)
    parts = lax.optimization_barrier(parts.astype(jnp.bfloat16)).astype(jnp.float32)
    return lax.optimization_barrier(jnp.sum(parts, axis=0))

def reference(spatial_qkv, temporal_qkv, cotangent, spatial_gate, temporal_gate, temporal_proj, live_counts):

    def one_group(accumulated, group_items):
        s_qkv, t_qkv, incoming, s_gate, t_gate, counts = group_items
        frame_ids = jnp.arange(FRAMES, dtype=jnp.int32)
        position_ids = jnp.arange(POS, dtype=jnp.int32)
        token_mask = ((frame_ids[:, None] < counts[0]) & (position_ids[None, :] < counts[1])).astype(jnp.float32)
        flowing = token_mask[:, :, None] * incoming.astype(jnp.float32)
        spatial_error = (flowing * s_gate).astype(jnp.bfloat16)
        temporal_error = (flowing * t_gate).astype(jnp.bfloat16)
        temporal_back = jnp.dot(temporal_error.reshape(FRAMES * POS, D), temporal_proj.T, preferred_element_type=jnp.float32).astype(jnp.bfloat16).reshape(FRAMES, POS, D)
        spatial_keep = jnp.broadcast_to(position_ids[None, :] < counts[1], (FRAMES, POS))
        spatial_out = attend(s_qkv[0], s_qkv[1], s_qkv[2], spatial_keep, 'bqhd,bkhd->bhqk', 'bhqk,bkhd->bqhd').astype(jnp.bfloat16)
        temporal_keep = jnp.broadcast_to(frame_ids[None, :] < counts[0], (POS, FRAMES))

        def temporal_attend(queries, key_block, value_block):
            return attend(queries, key_block, value_block, temporal_keep, 'qbhd,kbhd->bhqk', 'bhqk,kbhd->qbhd')
        temporal_result, pullback = jax.vjp(temporal_attend, t_qkv[0], t_qkv[1], t_qkv[2])
        temporal_out = temporal_result.astype(jnp.bfloat16)
        input_grads = jnp.stack(pullback(temporal_back.astype(jnp.float32)))
        spatial_sum = accumulated[0] + block_parts(spatial_out, spatial_error)
        temporal_sum = accumulated[1] + block_parts(temporal_out, temporal_error)
        return ((spatial_sum, temporal_sum), input_grads)
    start = (jnp.zeros((D, D), jnp.float32), jnp.zeros((D, D), jnp.float32))
    sums, all_grads = lax.scan(one_group, start, (spatial_qkv, temporal_qkv, cotangent, spatial_gate, temporal_gate, live_counts))
    return (all_grads, sums[0], sums[1])
```

```python
import functools
import jax
import jax.numpy as jnp
from jax import lax
from jax.experimental import pallas as pl
from jax.experimental.pallas import tpu as pltpu
from jax.sharding import PartitionSpec as P

HEADS = 16
HD = 72
LANES = 128
HALF = 640
SCALE = HD ** (-0.5)
NN = (((1,), (0,)), ((), ()))
NT = (((1,), (1,)), ((), ()))
TN = (((0,), (0,)), ((), ()))


def dot(left, right, dims):
    return lax.dot_general(left, right, dims, preferred_element_type=jnp.float32)


def head_tiles(head):
    return head * HD // LANES, ((head + 1) * HD + LANES - 1) // LANES


def head_lanes(head, first, last):
    lane = lax.broadcasted_iota(jnp.int32, (1, (last - first) * LANES), 1) + first * LANES
    return (lane >= head * HD) & (lane < (head + 1) * HD)


class Rows:
    def __init__(self, store):
        self.store = store
        self.open = {}

    def add(self, head, first, last, value, keep):
        for tile in range(first, last):
            at = slice((tile - first) * LANES, (tile - first + 1) * LANES)
            piece = value[:, at]
            if tile in self.open:
                piece = jnp.where(keep[:, at], piece, self.open[tile])
            self.open[tile] = piece
        done = (head + 1) * HD // LANES
        for tile in [t for t in self.open if t < done]:
            self.store(tile, self.open.pop(tile))


def softmax(scores):
    expo = jnp.exp(scores - jnp.max(scores, axis=-1, keepdims=True))
    return expo / jnp.sum(expo, axis=-1, keepdims=True)


def hand_over(core, out, error, mine, send):
    width = out.shape[-1]
    low, high = slice(0, HALF), slice(width - HALF, width)

    @pl.when(core == 0)
    def _():
        mine[...] = out[:, low]
        send[:, :HALF] = out[:, high]

    @pl.when(core == 1)
    def _():
        mine[...] = out[:, high]
        send[:, :HALF] = out[:, low]

    send[:, HALF:] = error


def spatial_kernel(counts, qkv, incoming, gate, mine, send, out):
    tokens, width = incoming.shape
    live_positions, frame_live, core = counts[1], counts[2], counts[4]
    keys_live = lax.broadcasted_iota(jnp.int32, (1, tokens), 1) < live_positions

    def store(tile, value):
        out[:, tile * LANES : (tile + 1) * LANES] = value.astype(jnp.bfloat16)

    rows = Rows(store)
    for head in range(HEADS):
        first, last = head_tiles(head)
        keep = head_lanes(head, first, last)
        at = slice(first * LANES, last * LANES)
        queries = jnp.where(keep, qkv[0, :, at], 0)
        scores = dot(queries, qkv[1, :, at], NT) * SCALE
        weights = softmax(jnp.where(keys_live, scores, -1e30)).astype(jnp.bfloat16)
        rows.add(head, first, last, dot(weights, qkv[2, :, at], NN), keep)
    token = lax.broadcasted_iota(jnp.int32, (tokens, 1), 0)
    live = ((token < live_positions) & (frame_live > 0)).astype(jnp.float32)
    error = (live * incoming[...].astype(jnp.float32) * gate[...]).astype(jnp.bfloat16)
    hand_over(core, out, error, mine, send)


def temporal_kernel(counts, arrived, gate, proj, grads, mine, send, error, back, out):
    frames, rows, width = arrived.shape
    positions = rows // 4
    tokens = frames * positions
    live_frames, core = counts[0], counts[4]
    live_positions = counts[1] - counts[3]
    token = lax.broadcasted_iota(jnp.int32, (tokens, 1), 0)
    live = (token // positions < live_frames) & (token % positions < live_positions)
    incoming = arrived[:, 3 * positions :, :].astype(jnp.float32).reshape(tokens, width)
    flowing = live.astype(jnp.float32) * incoming
    error[...] = (flowing * gate[...]).astype(jnp.bfloat16)
    back[...] = dot(error[...], proj[...], NT).astype(jnp.bfloat16)
    query = lax.broadcasted_iota(jnp.int32, (tokens, tokens), 0)
    key = lax.broadcasted_iota(jnp.int32, (tokens, tokens), 1)
    pairs = (query % positions == key % positions) & (key // positions < live_frames)

    def store_out(tile, value):
        out[:, tile * LANES : (tile + 1) * LANES] = value.astype(jnp.bfloat16)

    def store_grad(which):
        rows = slice(which * positions, (which + 1) * positions)

        def store(tile, value):
            at = slice(tile * LANES, (tile + 1) * LANES)
            grads[:, rows, at] = value.reshape(frames, positions, LANES).astype(jnp.bfloat16)

        return store

    def load(which, at):
        block = arrived[:, which * positions : (which + 1) * positions, at]
        return block.reshape(tokens, block.shape[-1])

    outs = Rows(store_out)
    to_q, to_k, to_v = (Rows(store_grad(i)) for i in range(3))
    for head in range(HEADS):
        first, last = head_tiles(head)
        keep = head_lanes(head, first, last)
        at = slice(first * LANES, last * LANES)
        q, k, v, b = load(0, at), load(1, at), load(2, at), back[:, at]
        scores = dot(jnp.where(keep, q, 0), k, NT) * SCALE
        weights = softmax(jnp.where(pairs, scores, -1e30))
        rounded = weights.astype(jnp.bfloat16)
        outs.add(head, first, last, dot(rounded, v, NN), keep)
        to_v.add(head, first, last, dot(rounded, b, TN), keep)
        reaching = dot(jnp.where(keep, b, 0), v, NT).astype(jnp.bfloat16).astype(jnp.float32)
        drop = jnp.sum(reaching * weights, axis=-1, keepdims=True)
        slope = (weights * (reaching - drop) * SCALE).astype(jnp.bfloat16)
        to_q.add(head, first, last, dot(slope, k, NN), keep)
        to_k.add(head, first, last, dot(slope, q, TN), keep)
    hand_over(core, out, error[...], mine, send)


def part_kernel(mine, send, came, part):
    total = dot(send[:, HALF:], mine[...], TN) + dot(came[:, HALF:], came[:, :HALF], TN)
    part[...] = total.astype(jnp.bfloat16).reshape(part.shape)


SM = pl.BlockSpec(memory_space=pltpu.SMEM)
VM = pl.BlockSpec(memory_space=pltpu.VMEM)


def shape(*dims):
    return jax.ShapeDtypeStruct(dims, jnp.bfloat16)


def cost(flops):
    return pl.CostEstimate(flops=flops, transcendentals=0, bytes_accessed=4_000_000)


def lines(major):
    side = round(lax.axis_size("dp") ** 0.5)
    if major:
        return [[x * side + z for x in range(side)] for z in range(side)]
    return [[x * side + z for z in range(side)] for x in range(side)]


def exchange(blocks, axis, groups=None):
    return lax.all_to_all(blocks, axis, split_axis=0, concat_axis=0, tiled=True, axis_index_groups=groups)


def scattered(part, by_permutes):
    side = part.shape[0]
    if not by_permutes:
        return lax.psum_scatter(part, "dp", scatter_dimension=0, tiled=True, axis_index_groups=lines(True))[0]
    here = lax.axis_index("dp") // side
    kept = lax.dynamic_index_in_dim(part, here, 0, keepdims=False)
    total = kept.astype(jnp.float32)
    for step in range(1, side):
        to = lambda i: (i // side + step) % side * side + i % side
        block = lax.dynamic_index_in_dim(part, (here + step) % side, 0, keepdims=False)
        came = lax.ppermute(block, "dp", [(i, to(i)) for i in range(side * side)])
        total = total + came.astype(jnp.float32)
    return total.astype(jnp.bfloat16)


def line_sum(mine, send, by_permutes):
    width = send.shape[1] - HALF
    side = len(lines(True))
    came = lax.ppermute(send, "seq", [(i, i ^ 1) for i in range(lax.axis_size("seq"))])
    part = pl.pallas_call(
        part_kernel,
        in_specs=[VM] * 3,
        out_specs=VM,
        out_shape=shape(side, width // side, HALF),
        cost_estimate=cost(2_000_000_000),
        name="part",
    )(mine, send, came)
    return scattered(part, by_permutes)


def body(spatial_qkv, temporal_qkv, cotangent, spatial_gate, temporal_gate, temporal_proj, live_counts):
    peers = lax.axis_size("seq")
    member = lax.axis_index("seq")
    core = member % 2
    incoming = cotangent[0, 0]
    tokens, width = incoming.shape
    positions = tokens // peers
    live_frames, live_positions = live_counts[0, 0], live_counts[0, 1]
    counts = jnp.stack(
        [live_frames, live_positions, (member < live_frames).astype(jnp.int32), member * positions, core]
    )
    blocks = jnp.concatenate([temporal_qkv[0, :, 0], cotangent[0]]).reshape(4, peers, positions, width)
    blocks = jnp.moveaxis(blocks, 1, 0).reshape(peers, 4 * positions, width)
    arrived = exchange(blocks, "seq")
    mine_s, send_s = pl.pallas_call(
        spatial_kernel,
        in_specs=[SM, VM, VM, VM],
        out_specs=[VM] * 2,
        out_shape=[shape(tokens, HALF), shape(tokens, HALF + width)],
        scratch_shapes=[pltpu.VMEM((tokens, width), jnp.bfloat16)],
        cost_estimate=cost(4_000_000_000),
        name="spatial",
    )(counts, spatial_qkv[0, :, 0], incoming, spatial_gate)
    grads, mine_t, send_t = pl.pallas_call(
        temporal_kernel,
        in_specs=[SM] + [VM] * 3,
        out_specs=[VM] * 3,
        out_shape=[shape(peers, 3 * positions, width), shape(tokens, HALF), shape(tokens, HALF + width)],
        scratch_shapes=[pltpu.VMEM((tokens, width), jnp.bfloat16)] * 3,
        cost_estimate=cost(8_000_000_000),
        name="temporal",
    )(counts, arrived, temporal_gate, temporal_proj)
    grads_home = exchange(grads, "seq")
    sums = jnp.stack([line_sum(mine_s, send_s, False), line_sum(mine_t, send_t, True)], axis=1)
    grads_home, sums = lax.optimization_barrier((grads_home, sums))
    grads_home = grads_home.reshape(peers, 3, positions, width)
    grads_home = jnp.moveaxis(grads_home, 1, 0).reshape(3, 1, tokens, width)
    side = len(lines(False))
    both = exchange(sums.reshape(side, -1, 2 * HALF), "dp", lines(False))
    both = both.astype(jnp.float32).sum(axis=0).reshape(-1, 2, HALF)
    kept = HEADS * HD // 2
    heads = jnp.where(core == 0, both[:, :, :kept], both[:, :, HALF - kept :])
    heads = heads.reshape(-1, 2, HEADS // 2, HD).transpose(2, 1, 0, 3)
    heads = jnp.concatenate([jnp.where(core == 0, heads, 0), jnp.where(core == 1, heads, 0)])
    rows = exchange(heads.reshape(HEADS, -1, HD), "seq").sum(axis=0).reshape(2, -1, HD)
    return (grads_home[None], rows[0].T, rows[1].T)


def solution(mesh):
    return jax.shard_map(
        body,
        mesh=mesh,
        in_specs=(
            P("dp", None, "seq", None, None),
            P("dp", None, "seq", None, None),
            P("dp", "seq", None, None),
            P("dp", None),
            P("dp", None),
            P(),
            P("dp", None),
        ),
        out_specs=(P("dp", None, "seq", None, None), P("seq", "dp"), P("seq", "dp")),
        check_vma=False,
    )
```

```python
import jax
import jax.numpy as jnp
from jax import lax
from jax.experimental import pallas as pl
from jax.experimental.pallas import tpu as pltpu
from jax.sharding import PartitionSpec as P


HEADS = 16
HD = 72
LANES = 128
HALF = 640
SCALE = HD ** (-0.5)
NN = (((1,), (0,)), ((), ()))
NT = (((1,), (1,)), ((), ()))
TN = (((0,), (0,)), ((), ()))


def dot(left, right, dims):
    return lax.dot_general(left, right, dims, preferred_element_type=jnp.float32)


def head_tiles(head):
    return head * HD // LANES, ((head + 1) * HD + LANES - 1) // LANES


def head_lanes(head, first, last):
    lane = lax.broadcasted_iota(jnp.int32, (1, (last - first) * LANES), 1) + first * LANES
    return (lane >= head * HD) & (lane < (head + 1) * HD)


class Rows:
    def __init__(self, store):
        self.store = store
        self.open = {}

    def add(self, head, first, last, value, keep):
        for tile in range(first, last):
            at = slice((tile - first) * LANES, (tile - first + 1) * LANES)
            piece = value[:, at]
            if tile in self.open:
                piece = jnp.where(keep[:, at], piece, self.open[tile])
            self.open[tile] = piece
        done = (head + 1) * HD // LANES
        for tile in [t for t in self.open if t < done]:
            self.store(tile, self.open.pop(tile))


def softmax(scores):
    expo = jnp.exp(scores - jnp.max(scores, axis=-1, keepdims=True))
    return expo / jnp.sum(expo, axis=-1, keepdims=True)


def hand_over(core, out, error, mine, send):
    width = out.shape[-1]
    low, high = slice(0, HALF), slice(width - HALF, width)

    @pl.when(core == 0)
    def _():
        mine[...] = out[:, low]
        send[:, :HALF] = out[:, high]

    @pl.when(core == 1)
    def _():
        mine[...] = out[:, high]
        send[:, :HALF] = out[:, low]

    send[:, HALF:] = error


def spatial_kernel(counts, qkv, incoming, gate, mine, send, out):
    tokens, _ = incoming.shape
    member = lax.axis_index("seq")
    live_positions = counts[0, 1]
    keys_live = lax.broadcasted_iota(jnp.int32, (1, tokens), 1) < live_positions

    def store(tile, value):
        out[:, tile * LANES : (tile + 1) * LANES] = value.astype(jnp.bfloat16)

    rows = Rows(store)
    for head in range(HEADS):
        first, last = head_tiles(head)
        keep = head_lanes(head, first, last)
        at = slice(first * LANES, last * LANES)
        queries = jnp.where(keep, qkv[0, :, at], 0)
        scores = dot(queries, qkv[1, :, at], NT) * SCALE
        weights = softmax(jnp.where(keys_live, scores, -1e30)).astype(jnp.bfloat16)
        rows.add(head, first, last, dot(weights, qkv[2, :, at], NN), keep)
    token = lax.broadcasted_iota(jnp.int32, (tokens, 1), 0)
    live = ((token < live_positions) & (member < counts[0, 0])).astype(jnp.float32)
    error = (live * incoming[...].astype(jnp.float32) * gate[...]).astype(jnp.bfloat16)
    hand_over(member % 2, out, error, mine, send)


class Block:
    def __init__(self, counts, arrived):
        self.arrived = arrived
        self.frames, rows, self.width = arrived.shape
        self.positions = rows // 4
        self.tokens = self.frames * self.positions
        query = lax.broadcasted_iota(jnp.int32, (self.tokens, self.tokens), 0)
        key = lax.broadcasted_iota(jnp.int32, (self.tokens, self.tokens), 1)
        same = query % self.positions == key % self.positions
        self.pairs = same & (key // self.positions < counts[0, 0])

    def load(self, which, at=slice(None)):
        block = self.arrived[:, which * self.positions : (which + 1) * self.positions, at]
        return block.reshape(self.tokens, block.shape[-1])

    def weights(self, at, keep):
        scores = dot(jnp.where(keep, self.load(0, at), 0), self.load(1, at), NT) * SCALE
        return softmax(jnp.where(self.pairs, scores, -1e30))


def forward_kernel(counts, arrived, gate, mine, send, out):
    block = Block(counts, arrived)
    member = lax.axis_index("seq")

    def store(tile, value):
        out[:, tile * LANES : (tile + 1) * LANES] = value.astype(jnp.bfloat16)

    rows = Rows(store)
    for head in range(HEADS):
        first, last = head_tiles(head)
        keep = head_lanes(head, first, last)
        at = slice(first * LANES, last * LANES)
        weights = block.weights(at, keep).astype(jnp.bfloat16)
        rows.add(head, first, last, dot(weights, block.load(2, at), NN), keep)
    token = lax.broadcasted_iota(jnp.int32, (block.tokens, 1), 0)
    place = token % block.positions + member * block.positions
    live = (token // block.positions < counts[0, 0]) & (place < counts[0, 1])
    flowing = live.astype(jnp.float32) * block.load(3).astype(jnp.float32)
    hand_over(member % 2, out, (flowing * gate[...]).astype(jnp.bfloat16), mine, send)


def backward_kernel(counts, arrived, send, proj, grads, back):
    block = Block(counts, arrived)
    back[...] = dot(send[:, HALF:], proj[...], NT).astype(jnp.bfloat16)

    def into(which):
        rows = slice(which * block.positions, (which + 1) * block.positions)

        def store(tile, value):
            value = value.reshape(block.frames, block.positions, LANES).astype(jnp.bfloat16)
            grads[:, rows, tile * LANES : (tile + 1) * LANES] = value

        return Rows(store)

    to_q, to_k, to_v = into(0), into(1), into(2)
    for head in range(HEADS):
        first, last = head_tiles(head)
        keep = head_lanes(head, first, last)
        at = slice(first * LANES, last * LANES)
        weights = block.weights(at, keep)
        b = back[:, at]
        to_v.add(head, first, last, dot(weights.astype(jnp.bfloat16), b, TN), keep)
        reaching = dot(jnp.where(keep, b, 0), block.load(2, at), NT)
        reaching = reaching.astype(jnp.bfloat16).astype(jnp.float32)
        drop = jnp.sum(reaching * weights, axis=-1, keepdims=True)
        slope = (weights * (reaching - drop) * SCALE).astype(jnp.bfloat16)
        to_q.add(head, first, last, dot(slope, block.load(1, at), NN), keep)
        to_k.add(head, first, last, dot(slope, block.load(0, at), TN), keep)


def part_kernel(mine, send, came, part):
    total = dot(send[:, HALF:], mine[...], TN) + dot(came[:, HALF:], came[:, :HALF], TN)
    part[...] = total.astype(jnp.bfloat16).reshape(part.shape)


SM = pl.BlockSpec(memory_space=pltpu.SMEM)
VM = pl.BlockSpec(memory_space=pltpu.VMEM)


def shape(*dims):
    return jax.ShapeDtypeStruct(dims, jnp.bfloat16)


def cost(flops):
    return pl.CostEstimate(flops=flops, transcendentals=0, bytes_accessed=4_000_000)


def lines(major):
    side = round(lax.axis_size("dp") ** 0.5)
    if major:
        return [[x * side + z for x in range(side)] for z in range(side)]
    return [[x * side + z for z in range(side)] for x in range(side)]


def exchange(blocks, axis, groups=None):
    return lax.all_to_all(blocks, axis, split_axis=0, concat_axis=0, tiled=True, axis_index_groups=groups)


def shifts(blocks, axis, here, peers, to):
    came = [lax.dynamic_index_in_dim(blocks, here, 0, keepdims=False)]
    count = lax.axis_size(axis)
    for step in range(1, peers):
        block = lax.dynamic_index_in_dim(blocks, (here + step) % peers, 0, keepdims=False)
        came.append(lax.ppermute(block, axis, [(i, to(i, step)) for i in range(count)]))
    return came


def summed(blocks):
    total = blocks[0].astype(jnp.float32)
    for block in blocks[1:]:
        total = total + block.astype(jnp.float32)
    return total


def part_of(mine, send):
    width = send.shape[1] - HALF
    side = len(lines(True))
    came = lax.ppermute(send, "seq", [(i, i ^ 1) for i in range(lax.axis_size("seq"))])
    return pl.pallas_call(
        part_kernel,
        in_specs=[VM] * 3,
        out_specs=VM,
        out_shape=shape(side, width // side, HALF),
        cost_estimate=cost(2_000_000_000),
        name="part",
    )(mine, send, came)


def body(spatial_qkv, temporal_qkv, cotangent, spatial_gate, temporal_gate, temporal_proj, live_counts):
    peers = lax.axis_size("seq")
    member = lax.axis_index("seq")
    core = member % 2
    incoming = cotangent[0, 0]
    tokens, width = incoming.shape
    positions = tokens // peers
    side = len(lines(True))
    x, z = lax.axis_index("dp") // side, lax.axis_index("dp") % side
    along_x = lambda i, n: (i // side + n) % side * side + i % side
    along_z = lambda i, n: i // side * side + (i % side + n) % side
    blocks = jnp.concatenate([temporal_qkv[0, :, 0], cotangent[0]]).reshape(4, peers, positions, width)
    blocks = jnp.moveaxis(blocks, 1, 0).reshape(peers, 4 * positions, width)
    arrived = exchange(blocks, "seq")
    handed = [shape(tokens, HALF), shape(tokens, HALF + width)]
    kept_out = [pltpu.VMEM((tokens, width), jnp.bfloat16)]
    mine_s, send_s = pl.pallas_call(
        spatial_kernel,
        in_specs=[SM, VM, VM, VM],
        out_specs=[VM] * 2,
        out_shape=handed,
        scratch_shapes=kept_out,
        cost_estimate=cost(4_000_000_000),
        name="spatial",
    )(live_counts, spatial_qkv[0, :, 0], incoming, spatial_gate)
    part_s = part_of(mine_s, send_s)
    came_s = shifts(part_s, "dp", x, side, along_x)
    mine_t, send_t = pl.pallas_call(
        forward_kernel,
        in_specs=[SM, VM, VM],
        out_specs=[VM] * 2,
        out_shape=handed,
        scratch_shapes=kept_out,
        cost_estimate=cost(4_000_000_000),
        name="forward",
    )(live_counts, arrived, temporal_gate)
    part_t = part_of(mine_t, send_t)
    came_t = shifts(part_t, "dp", x, side, along_x)
    grads = pl.pallas_call(
        backward_kernel,
        in_specs=[SM, VM, VM, VM],
        out_specs=VM,
        out_shape=shape(peers, 3 * positions, width),
        scratch_shapes=kept_out,
        cost_estimate=cost(8_000_000_000),
        name="backward",
    )(live_counts, arrived, send_t, temporal_proj)
    home = exchange(grads, "seq")
    sums = jnp.concatenate([summed(came_s), summed(came_t)], axis=1).astype(jnp.bfloat16)
    came = shifts(sums.reshape(side, -1, 2 * HALF), "dp", z, side, along_z)
    both = summed(came).reshape(-1, 2, HALF)
    kept = HEADS * HD // 2
    heads = jnp.where(core == 0, both[:, :, :kept], both[:, :, HALF - kept :])
    heads = heads.reshape(-1, 2, HEADS // 2, HD).transpose(2, 1, 0, 3)
    heads = jnp.concatenate([jnp.where(core == 0, heads, 0), jnp.where(core == 1, heads, 0)])
    home, heads = lax.optimization_barrier((home, heads))
    home = jnp.moveaxis(home.reshape(peers, 3, positions, width), 1, 0).reshape(3, 1, tokens, width)
    rows = exchange(heads.reshape(HEADS, -1, HD), "seq").sum(axis=0).reshape(2, -1, HD)
    return (home[None], rows[0].T, rows[1].T)


def solution(mesh):
    return jax.shard_map(
        body,
        mesh=mesh,
        in_specs=(
            P("dp", None, "seq", None, None),
            P("dp", None, "seq", None, None),
            P("dp", "seq", None, None),
            P("dp", None),
            P("dp", None),
            P(),
            P("dp", None),
        ),
        out_specs=(P("dp", None, "seq", None, None), P("seq", "dp"), P("seq", "dp")),
        check_vma=False,
    )
```

```python
import jax
import jax.numpy as jnp
from jax import lax
from jax.experimental import pallas as pl
from jax.experimental.pallas import tpu as pltpu
from jax.sharding import PartitionSpec as P


HEADS = 16
HD = 72
LANES = 128
HALF = 640
SCALE = HD ** (-0.5)
NN = (((1,), (0,)), ((), ()))
NT = (((1,), (1,)), ((), ()))
TN = (((0,), (0,)), ((), ()))


def dot(left, right, dims):
    return lax.dot_general(left, right, dims, preferred_element_type=jnp.float32)


def head_tiles(head):
    return head * HD // LANES, ((head + 1) * HD + LANES - 1) // LANES


def head_lanes(head, first, last):
    lane = lax.broadcasted_iota(jnp.int32, (1, (last - first) * LANES), 1) + first * LANES
    return (lane >= head * HD) & (lane < (head + 1) * HD)


class Rows:
    def __init__(self, store):
        self.store = store
        self.open = {}

    def add(self, head, first, last, value, keep):
        for tile in range(first, last):
            at = slice((tile - first) * LANES, (tile - first + 1) * LANES)
            piece = value[:, at]
            if tile in self.open:
                piece = jnp.where(keep[:, at], piece, self.open[tile])
            self.open[tile] = piece
        done = (head + 1) * HD // LANES
        for tile in [t for t in self.open if t < done]:
            self.store(tile, self.open.pop(tile))


class Shares:
    def __init__(self, shares):
        self.shares = shares
        self.open = {}

    def add(self, head, first, last, value, keep):
        value = jnp.where(keep, value, 0)
        if last - first == 1:
            value = jnp.concatenate([value, jnp.zeros_like(value)], axis=1)
        core, slot = head % 2, head // 2
        goal = slot * HD // LANES
        shift = (slot * HD - goal * LANES) - (head * HD - first * LANES)
        if shift:
            value = pltpu.roll(value, shift % (2 * LANES), 1)
        for tile in range(goal, ((slot + 1) * HD + LANES - 1) // LANES):
            piece = value[:, (tile - goal) * LANES : (tile - goal + 1) * LANES]
            if (core, tile) in self.open:
                piece = piece + self.open[core, tile]
            self.open[core, tile] = piece
        done = (slot + 1) * HD // LANES if slot + 1 < HEADS // 2 else HALF // LANES
        for key in [k for k in self.open if k[0] == core and k[1] < done]:
            lanes = slice(key[1] * LANES, (key[1] + 1) * LANES)
            self.shares[core, :, lanes] = self.open.pop(key).astype(jnp.bfloat16)


def softmax(scores):
    expo = jnp.exp(scores - jnp.max(scores, axis=-1, keepdims=True))
    return expo / jnp.sum(expo, axis=-1, keepdims=True)


def hand_over(core, shares, error, mine, send):
    mine[...] = shares[core]
    send[:, :HALF] = shares[1 - core]
    send[:, HALF:] = error


def spatial_kernel(counts, qkv, incoming, gate, mine, send, out):
    tokens, _ = incoming.shape
    member = lax.axis_index("seq")
    live_positions = counts[0, 1]
    keys_live = lax.broadcasted_iota(jnp.int32, (1, tokens), 1) < live_positions

    rows = Shares(out)
    for head in range(HEADS):
        first, last = head_tiles(head)
        keep = head_lanes(head, first, last)
        at = slice(first * LANES, last * LANES)
        queries = jnp.where(keep, qkv[0, :, at], 0)
        scores = dot(queries, qkv[1, :, at], NT) * SCALE
        weights = softmax(jnp.where(keys_live, scores, -1e30)).astype(jnp.bfloat16)
        rows.add(head, first, last, dot(weights, qkv[2, :, at], NN), keep)
    token = lax.broadcasted_iota(jnp.int32, (tokens, 1), 0)
    live = ((token < live_positions) & (member < counts[0, 0])).astype(jnp.float32)
    error = (live * incoming[...].astype(jnp.float32) * gate[...]).astype(jnp.bfloat16)
    hand_over(member % 2, out, error, mine, send)


class Block:
    def __init__(self, counts, arrived):
        self.arrived = arrived
        self.frames, rows, self.width = arrived.shape
        self.positions = rows // 4
        self.tokens = self.frames * self.positions
        query = lax.broadcasted_iota(jnp.int32, (self.tokens, self.tokens), 0)
        key = lax.broadcasted_iota(jnp.int32, (self.tokens, self.tokens), 1)
        same = query % self.positions == key % self.positions
        self.pairs = same & (key // self.positions < counts[0, 0])

    def load(self, which, at=slice(None)):
        block = self.arrived[:, which * self.positions : (which + 1) * self.positions, at]
        return block.reshape(self.tokens, block.shape[-1])

    def weights(self, at, keep):
        scores = dot(jnp.where(keep, self.load(0, at), 0), self.load(1, at), NT) * SCALE
        return softmax(jnp.where(self.pairs, scores, -1e30))


def forward_kernel(counts, arrived, gate, mine, send, out):
    block = Block(counts, arrived)
    member = lax.axis_index("seq")

    rows = Shares(out)
    for head in range(HEADS):
        first, last = head_tiles(head)
        keep = head_lanes(head, first, last)
        at = slice(first * LANES, last * LANES)
        weights = block.weights(at, keep).astype(jnp.bfloat16)
        rows.add(head, first, last, dot(weights, block.load(2, at), NN), keep)
    token = lax.broadcasted_iota(jnp.int32, (block.tokens, 1), 0)
    place = token % block.positions + member * block.positions
    live = (token // block.positions < counts[0, 0]) & (place < counts[0, 1])
    flowing = live.astype(jnp.float32) * block.load(3).astype(jnp.float32)
    hand_over(member % 2, out, (flowing * gate[...]).astype(jnp.bfloat16), mine, send)


def backward_kernel(counts, arrived, send, proj, grads, back):
    block = Block(counts, arrived)
    back[...] = dot(send[:, HALF:], proj[...], NT).astype(jnp.bfloat16)

    def into(which):
        rows = slice(which * block.positions, (which + 1) * block.positions)

        def store(tile, value):
            value = value.reshape(block.frames, block.positions, LANES).astype(jnp.bfloat16)
            grads[:, rows, tile * LANES : (tile + 1) * LANES] = value

        return Rows(store)

    to_q, to_k, to_v = into(0), into(1), into(2)
    for head in range(HEADS):
        first, last = head_tiles(head)
        keep = head_lanes(head, first, last)
        at = slice(first * LANES, last * LANES)
        weights = block.weights(at, keep)
        b = back[:, at]
        to_v.add(head, first, last, dot(weights.astype(jnp.bfloat16), b, TN), keep)
        reaching = dot(jnp.where(keep, b, 0), block.load(2, at), NT)
        reaching = reaching.astype(jnp.bfloat16).astype(jnp.float32)
        drop = jnp.sum(reaching * weights, axis=-1, keepdims=True)
        slope = (weights * (reaching - drop) * SCALE).astype(jnp.bfloat16)
        to_q.add(head, first, last, dot(slope, block.load(1, at), NN), keep)
        to_k.add(head, first, last, dot(slope, block.load(0, at), TN), keep)


def part_kernel(mine, send, came, part):
    total = dot(send[:, HALF:], mine[...], TN) + dot(came[:, HALF:], came[:, :HALF], TN)
    part[...] = total.astype(jnp.bfloat16).reshape(part.shape)


SM = pl.BlockSpec(memory_space=pltpu.SMEM)
VM = pl.BlockSpec(memory_space=pltpu.VMEM)


def shape(*dims):
    return jax.ShapeDtypeStruct(dims, jnp.bfloat16)


def cost(flops):
    return pl.CostEstimate(flops=flops, transcendentals=0, bytes_accessed=4_000_000)


def lines(major):
    side = round(lax.axis_size("dp") ** 0.5)
    if major:
        return [[x * side + z for x in range(side)] for z in range(side)]
    return [[x * side + z for z in range(side)] for x in range(side)]


def near(array):
    return pltpu.with_memory_space_constraint(array, pltpu.VMEM)


def exchange(blocks, axis, groups=None):
    return lax.all_to_all(blocks, axis, split_axis=0, concat_axis=0, tiled=True, axis_index_groups=groups)


def shifts(blocks, axis, here, peers, to):
    came = [lax.dynamic_index_in_dim(blocks, here, 0, keepdims=False)]
    count = lax.axis_size(axis)
    for step in range(1, peers):
        block = lax.dynamic_index_in_dim(blocks, (here + step) % peers, 0, keepdims=False)
        came.append(lax.ppermute(block, axis, [(i, to(i, step)) for i in range(count)]))
    return came


def summed(blocks):
    total = blocks[0].astype(jnp.float32)
    for block in blocks[1:]:
        total = total + block.astype(jnp.float32)
    return total


def part_of(mine, send):
    width = send.shape[1] - HALF
    side = len(lines(True))
    came = lax.ppermute(send, "seq", [(i, i ^ 1) for i in range(lax.axis_size("seq"))])
    return pl.pallas_call(
        part_kernel,
        in_specs=[VM] * 3,
        out_specs=VM,
        out_shape=shape(side, width // side, HALF),
        cost_estimate=cost(2_000_000_000),
        name="part",
    )(mine, send, came)


def body(spatial_qkv, temporal_qkv, cotangent, spatial_gate, temporal_gate, temporal_proj, live_counts):
    peers = lax.axis_size("seq")
    incoming = cotangent[0, 0]
    tokens, width = incoming.shape
    positions = tokens // peers
    side = len(lines(True))
    x, z = lax.axis_index("dp") // side, lax.axis_index("dp") % side
    along_x = lambda i, n: (i // side + n) % side * side + i % side
    along_z = lambda i, n: i // side * side + (i % side + n) % side
    blocks = jnp.concatenate([temporal_qkv[0, :, 0], cotangent[0]]).reshape(4, peers, positions, width)
    blocks = jnp.moveaxis(blocks, 1, 0).reshape(peers, 4 * positions, width)
    arrived = near(exchange(blocks, "seq"))
    handed = [shape(tokens, HALF), shape(tokens, HALF + width)]
    shares = [pltpu.VMEM((2, tokens, HALF), jnp.bfloat16)]
    mine_s, send_s = pl.pallas_call(
        spatial_kernel,
        in_specs=[SM, VM, VM, VM],
        out_specs=[VM] * 2,
        out_shape=handed,
        scratch_shapes=shares,
        cost_estimate=cost(4_000_000_000),
        name="spatial",
    )(live_counts, near(spatial_qkv[0, :, 0]), near(incoming), spatial_gate)
    part_s = part_of(mine_s, send_s)
    came_s = shifts(part_s, "dp", x, side, along_x)
    mine_t, send_t = pl.pallas_call(
        forward_kernel,
        in_specs=[SM, VM, VM],
        out_specs=[VM] * 2,
        out_shape=handed,
        scratch_shapes=shares,
        cost_estimate=cost(4_000_000_000),
        name="forward",
    )(live_counts, arrived, temporal_gate)
    part_t = part_of(mine_t, send_t)
    came_t = exchange(part_t, "dp", lines(True))
    grads = pl.pallas_call(
        backward_kernel,
        in_specs=[SM, VM, VM, VM],
        out_specs=VM,
        out_shape=shape(peers, 3 * positions, width),
        scratch_shapes=[pltpu.VMEM((tokens, width), jnp.bfloat16)],
        cost_estimate=cost(8_000_000_000),
        name="backward",
    )(live_counts, arrived, send_t, temporal_proj)
    came_t, grads = lax.optimization_barrier((came_t, grads))
    home = exchange(grads, "seq")
    sum_t = summed([came_t[i] for i in range(side)])
    sums = jnp.concatenate([summed(came_s), sum_t], axis=1).astype(jnp.bfloat16)
    came = shifts(sums.reshape(side, -1, 2 * HALF), "dp", z, side, along_z)
    both = summed(came).reshape(-1, 2, HALF)
    heads = both[:, :, : HEADS // 2 * HD].reshape(-1, 2, HEADS // 2, HD).transpose(2, 1, 0, 3)
    heads = heads.reshape(HEADS // 2, -1, HD)
    home, heads = lax.optimization_barrier((home, heads))
    home = jnp.moveaxis(home.reshape(peers, 3, positions, width), 1, 0).reshape(3, 1, tokens, width)
    chips = [[i for i in range(peers) if i % 2 == c] for c in range(2)]
    rows = exchange(heads, "seq", chips).sum(axis=0).reshape(2, -1, HD)
    return (home[None], rows[0].T, rows[1].T)


def solution(mesh):
    return jax.shard_map(
        body,
        mesh=mesh,
        in_specs=(
            P("dp", None, "seq", None, None),
            P("dp", None, "seq", None, None),
            P("dp", "seq", None, None),
            P("dp", None),
            P("dp", None),
            P(),
            P("dp", None),
        ),
        out_specs=(P("dp", None, "seq", None, None), P("seq", "dp"), P("seq", "dp")),
        check_vma=False,
    )
```

```python
import jax
import jax.numpy as jnp
from jax import lax
from jax.experimental import pallas as pl
from jax.experimental.pallas import tpu as pltpu
from jax.sharding import PartitionSpec as P


HEADS = 16
HD = 72
LANES = 128
HALF = 640
SCALE = HD ** (-0.5)
NN = (((1,), (0,)), ((), ()))
NT = (((1,), (1,)), ((), ()))
TN = (((0,), (0,)), ((), ()))


def dot(left, right, dims):
    return lax.dot_general(left, right, dims, preferred_element_type=jnp.float32)


def head_tiles(head):
    return head * HD // LANES, ((head + 1) * HD + LANES - 1) // LANES


def head_lanes(head, first, last):
    lane = lax.broadcasted_iota(jnp.int32, (1, (last - first) * LANES), 1) + first * LANES
    return (lane >= head * HD) & (lane < (head + 1) * HD)


class Rows:
    def __init__(self, store):
        self.store = store
        self.open = {}

    def add(self, head, first, last, value, keep):
        for tile in range(first, last):
            at = slice((tile - first) * LANES, (tile - first + 1) * LANES)
            piece = value[:, at]
            if tile in self.open:
                piece = jnp.where(keep[:, at], piece, self.open[tile])
            self.open[tile] = piece
        done = (head + 1) * HD // LANES
        for tile in [t for t in self.open if t < done]:
            self.store(tile, self.open.pop(tile))


class Shares:
    def __init__(self, shares):
        self.shares = shares
        self.open = {}

    def add(self, head, first, last, value, keep):
        value = jnp.where(keep, value, 0)
        if last - first == 1:
            value = jnp.concatenate([value, jnp.zeros_like(value)], axis=1)
        core, slot = head % 2, head // 2
        goal = slot * HD // LANES
        shift = (slot * HD - goal * LANES) - (head * HD - first * LANES)
        if shift:
            value = pltpu.roll(value, shift % (2 * LANES), 1)
        for tile in range(goal, ((slot + 1) * HD + LANES - 1) // LANES):
            piece = value[:, (tile - goal) * LANES : (tile - goal + 1) * LANES]
            if (core, tile) in self.open:
                piece = piece + self.open[core, tile]
            self.open[core, tile] = piece
        done = (slot + 1) * HD // LANES if slot + 1 < HEADS // 2 else HALF // LANES
        for key in [k for k in self.open if k[0] == core and k[1] < done]:
            lanes = slice(key[1] * LANES, (key[1] + 1) * LANES)
            self.shares[core, :, lanes] = self.open.pop(key).astype(jnp.bfloat16)


def softmax(scores):
    expo = jnp.exp(scores - jnp.max(scores, axis=-1, keepdims=True))
    return expo / jnp.sum(expo, axis=-1, keepdims=True)


def hand_over(core, shares, error, mine, send):
    mine[...] = shares[core]
    send[:, :HALF] = shares[1 - core]
    send[:, HALF:] = error


def spatial_kernel(counts, qkv, incoming, gate, mine, send, out):
    tokens, _ = incoming.shape
    member = lax.axis_index("seq")
    live_positions = counts[0, 1]
    keys_live = lax.broadcasted_iota(jnp.int32, (1, tokens), 1) < live_positions

    rows = Shares(out)
    for head in range(HEADS):
        first, last = head_tiles(head)
        keep = head_lanes(head, first, last)
        at = slice(first * LANES, last * LANES)
        queries = jnp.where(keep, qkv[0, :, at], 0)
        scores = dot(queries, qkv[1, :, at], NT) * SCALE
        weights = softmax(jnp.where(keys_live, scores, -1e30)).astype(jnp.bfloat16)
        rows.add(head, first, last, dot(weights, qkv[2, :, at], NN), keep)
    token = lax.broadcasted_iota(jnp.int32, (tokens, 1), 0)
    live = ((token < live_positions) & (member < counts[0, 0])).astype(jnp.float32)
    error = (live * incoming[...].astype(jnp.float32) * gate[...]).astype(jnp.bfloat16)
    hand_over(member % 2, out, error, mine, send)


class Block:
    def __init__(self, counts, arrived):
        self.arrived = arrived
        self.frames, rows, self.width = arrived.shape
        self.positions = rows // 4
        self.tokens = self.frames * self.positions
        query = lax.broadcasted_iota(jnp.int32, (self.tokens, self.tokens), 0)
        key = lax.broadcasted_iota(jnp.int32, (self.tokens, self.tokens), 1)
        same = query % self.positions == key % self.positions
        self.pairs = same & (key // self.positions < counts[0, 0])

    def load(self, which, at=slice(None)):
        block = self.arrived[:, which * self.positions : (which + 1) * self.positions, at]
        return block.reshape(self.tokens, block.shape[-1])

    def weights(self, at, keep):
        scores = dot(jnp.where(keep, self.load(0, at), 0), self.load(1, at), NT) * SCALE
        return softmax(jnp.where(self.pairs, scores, -1e30))


def forward_kernel(counts, arrived, gate, mine, send, out):
    block = Block(counts, arrived)
    member = lax.axis_index("seq")

    rows = Shares(out)
    for head in range(HEADS):
        first, last = head_tiles(head)
        keep = head_lanes(head, first, last)
        at = slice(first * LANES, last * LANES)
        weights = block.weights(at, keep).astype(jnp.bfloat16)
        rows.add(head, first, last, dot(weights, block.load(2, at), NN), keep)
    token = lax.broadcasted_iota(jnp.int32, (block.tokens, 1), 0)
    place = token % block.positions + member * block.positions
    live = (token // block.positions < counts[0, 0]) & (place < counts[0, 1])
    flowing = live.astype(jnp.float32) * block.load(3).astype(jnp.float32)
    hand_over(member % 2, out, (flowing * gate[...]).astype(jnp.bfloat16), mine, send)


def backward_kernel(counts, arrived, send, proj, grads, back):
    block = Block(counts, arrived)
    back[...] = dot(send[:, HALF:], proj[...], NT).astype(jnp.bfloat16)

    def into(which):
        rows = slice(which * block.positions, (which + 1) * block.positions)

        def store(tile, value):
            value = value.reshape(block.frames, block.positions, LANES).astype(jnp.bfloat16)
            grads[:, rows, tile * LANES : (tile + 1) * LANES] = value

        return Rows(store)

    to_q, to_k, to_v = into(0), into(1), into(2)
    for head in range(HEADS):
        first, last = head_tiles(head)
        keep = head_lanes(head, first, last)
        at = slice(first * LANES, last * LANES)
        weights = block.weights(at, keep)
        b = back[:, at]
        to_v.add(head, first, last, dot(weights.astype(jnp.bfloat16), b, TN), keep)
        reaching = dot(jnp.where(keep, b, 0), block.load(2, at), NT)
        reaching = reaching.astype(jnp.bfloat16).astype(jnp.float32)
        drop = jnp.sum(reaching * weights, axis=-1, keepdims=True)
        slope = (weights * (reaching - drop) * SCALE).astype(jnp.bfloat16)
        to_q.add(head, first, last, dot(slope, block.load(1, at), NN), keep)
        to_k.add(head, first, last, dot(slope, block.load(0, at), TN), keep)


def chip_part(mine, send, came):
    return dot(send[:, HALF:], mine[...], TN) + dot(came[:, HALF:], came[:, :HALF], TN)


def part_x_kernel(mine, send, came, part):
    part[...] = chip_part(mine, send, came).astype(jnp.bfloat16).reshape(part.shape)


def part_z_kernel(mine, send, came, part, total, block):
    side = part.shape[0]
    rows = total.shape[0] // side**2
    total[...] = chip_part(mine, send, came)
    for z in range(side):
        for x in range(side):
            start = (x * side + z) * rows
            block[x * rows : (x + 1) * rows, :] = total[start : start + rows, :]
        part[z] = block[...].astype(jnp.bfloat16)


SM = pl.BlockSpec(memory_space=pltpu.SMEM)
VM = pl.BlockSpec(memory_space=pltpu.VMEM)


def shape(*dims):
    return jax.ShapeDtypeStruct(dims, jnp.bfloat16)


def cost(flops):
    return pl.CostEstimate(flops=flops, transcendentals=0, bytes_accessed=4_000_000)


def lines(major):
    side = round(lax.axis_size("dp") ** 0.5)
    if major:
        return [[x * side + z for x in range(side)] for z in range(side)]
    return [[x * side + z for z in range(side)] for x in range(side)]


def near(array):
    return pltpu.with_memory_space_constraint(array, pltpu.VMEM)


def exchange(blocks, axis, groups=None):
    return lax.all_to_all(blocks, axis, split_axis=0, concat_axis=0, tiled=True, axis_index_groups=groups)


def shifts(blocks, axis, here, peers, to):
    came = [lax.dynamic_index_in_dim(blocks, here, 0, keepdims=False)]
    count = lax.axis_size(axis)
    for step in range(1, peers):
        block = lax.dynamic_index_in_dim(blocks, (here + step) % peers, 0, keepdims=False)
        came.append(lax.ppermute(block, axis, [(i, to(i, step)) for i in range(count)]))
    return came


def summed(blocks):
    total = blocks[0].astype(jnp.float32)
    for block in blocks[1:]:
        total = total + block.astype(jnp.float32)
    return total


def part_of(mine, send, z_first):
    width = send.shape[1] - HALF
    side = len(lines(True))
    came = lax.ppermute(send, "seq", [(i, i ^ 1) for i in range(lax.axis_size("seq"))])
    scratch = [pltpu.VMEM((width, HALF), jnp.float32), pltpu.VMEM((width // side, HALF), jnp.float32)]
    return pl.pallas_call(
        part_z_kernel if z_first else part_x_kernel,
        in_specs=[VM] * 3,
        out_specs=VM,
        out_shape=shape(side, width // side, HALF),
        scratch_shapes=scratch if z_first else [],
        cost_estimate=cost(2_000_000_000),
        name="part_z" if z_first else "part_x",
    )(mine, send, came)


def body(spatial_qkv, temporal_qkv, cotangent, spatial_gate, temporal_gate, temporal_proj, live_counts):
    peers = lax.axis_size("seq")
    incoming = cotangent[0, 0]
    tokens, width = incoming.shape
    positions = tokens // peers
    side = len(lines(True))
    z = lax.axis_index("dp") % side
    along_z = lambda i, n: i // side * side + (i % side + n) % side
    blocks = jnp.concatenate([temporal_qkv[0, :, 0], cotangent[0]]).reshape(4, peers, positions, width)
    blocks = jnp.moveaxis(blocks, 1, 0).reshape(peers, 4 * positions, width)
    arrived = near(exchange(blocks, "seq"))
    handed = [shape(tokens, HALF), shape(tokens, HALF + width)]
    shares = [pltpu.VMEM((2, tokens, HALF), jnp.bfloat16)]
    mine_s, send_s = pl.pallas_call(
        spatial_kernel,
        in_specs=[SM, VM, VM, VM],
        out_specs=[VM] * 2,
        out_shape=handed,
        scratch_shapes=shares,
        cost_estimate=cost(4_000_000_000),
        name="spatial",
    )(live_counts, near(spatial_qkv[0, :, 0]), near(incoming), spatial_gate)
    came_s = shifts(part_of(mine_s, send_s, True), "dp", z, side, along_z)
    mine_t, send_t = pl.pallas_call(
        forward_kernel,
        in_specs=[SM, VM, VM],
        out_specs=[VM] * 2,
        out_shape=handed,
        scratch_shapes=shares,
        cost_estimate=cost(4_000_000_000),
        name="forward",
    )(live_counts, arrived, temporal_gate)
    part_t = part_of(mine_t, send_t, False)
    came_t = exchange(part_t, "dp", lines(True))
    grads = pl.pallas_call(
        backward_kernel,
        in_specs=[SM, VM, VM, VM],
        out_specs=VM,
        out_shape=shape(peers, 3 * positions, width),
        scratch_shapes=[pltpu.VMEM((tokens, width), jnp.bfloat16)],
        cost_estimate=cost(8_000_000_000),
        name="backward",
    )(live_counts, arrived, send_t, temporal_proj)
    came_t, grads = lax.optimization_barrier((came_t, grads))
    home = exchange(grads, "seq")
    sum_t = summed([came_t[i] for i in range(side)]).astype(jnp.bfloat16)
    came_t = shifts(sum_t.reshape(side, -1, HALF), "dp", z, side, along_z)
    sum_s = summed(came_s).astype(jnp.bfloat16)
    home, sum_s = lax.optimization_barrier((home, sum_s))
    came_s = exchange(sum_s.reshape(side, -1, HALF), "dp", lines(True))
    both = jnp.stack([came_s.astype(jnp.float32).sum(axis=0), summed(came_t)], axis=1)
    heads = both[:, :, : HEADS // 2 * HD].reshape(-1, 2, HEADS // 2, HD).transpose(2, 1, 0, 3)
    heads = heads.reshape(HEADS // 2, -1, HD)
    home = jnp.moveaxis(home.reshape(peers, 3, positions, width), 1, 0).reshape(3, 1, tokens, width)
    chips = [[i for i in range(peers) if i % 2 == c] for c in range(2)]
    rows = exchange(heads, "seq", chips).sum(axis=0).reshape(2, -1, HD)
    return (home[None], rows[0].T, rows[1].T)


def solution(mesh):
    return jax.shard_map(
        body,
        mesh=mesh,
        in_specs=(
            P("dp", None, "seq", None, None),
            P("dp", None, "seq", None, None),
            P("dp", "seq", None, None),
            P("dp", None),
            P("dp", None),
            P(),
            P("dp", None),
        ),
        out_specs=(P("dp", None, "seq", None, None), P("seq", "dp"), P("seq", "dp")),
        check_vma=False,
    )
```

```python
import jax
import jax.numpy as jnp
from jax import lax
from jax.experimental import pallas as pl
from jax.experimental.pallas import tpu as pltpu
from jax.sharding import PartitionSpec as P


HEADS = 16
HD = 72
LANES = 128
HALF = 640
SCALE = HD ** (-0.5)
NN = (((1,), (0,)), ((), ()))
NT = (((1,), (1,)), ((), ()))
TN = (((0,), (0,)), ((), ()))


def dot(left, right, dims):
    return lax.dot_general(left, right, dims, preferred_element_type=jnp.float32)


def head_tiles(head):
    return head * HD // LANES, ((head + 1) * HD + LANES - 1) // LANES


def head_lanes(head, first, last):
    lane = lax.broadcasted_iota(jnp.int32, (1, (last - first) * LANES), 1) + first * LANES
    return (lane >= head * HD) & (lane < (head + 1) * HD)


class Rows:
    def __init__(self, store):
        self.store = store
        self.open = {}

    def add(self, head, first, last, value, keep):
        for tile in range(first, last):
            at = slice((tile - first) * LANES, (tile - first + 1) * LANES)
            piece = value[:, at]
            if tile in self.open:
                piece = jnp.where(keep[:, at], piece, self.open[tile])
            self.open[tile] = piece
        done = (head + 1) * HD // LANES
        for tile in [t for t in self.open if t < done]:
            self.store(tile, self.open.pop(tile))


class Shares:
    def __init__(self, shares):
        self.shares = shares
        self.open = {}

    def add(self, head, first, last, value, keep):
        value = jnp.where(keep, value, 0)
        if last - first == 1:
            value = jnp.concatenate([value, jnp.zeros_like(value)], axis=1)
        core, slot = head % 2, head // 2
        goal = slot * HD // LANES
        shift = (slot * HD - goal * LANES) - (head * HD - first * LANES)
        if shift:
            value = pltpu.roll(value, shift % (2 * LANES), 1)
        for tile in range(goal, ((slot + 1) * HD + LANES - 1) // LANES):
            piece = value[:, (tile - goal) * LANES : (tile - goal + 1) * LANES]
            if (core, tile) in self.open:
                piece = piece + self.open[core, tile]
            self.open[core, tile] = piece
        done = (slot + 1) * HD // LANES if slot + 1 < HEADS // 2 else HALF // LANES
        for key in [k for k in self.open if k[0] == core and k[1] < done]:
            lanes = slice(key[1] * LANES, (key[1] + 1) * LANES)
            self.shares[core, :, lanes] = self.open.pop(key).astype(jnp.bfloat16)


def softmax(scores):
    expo = jnp.exp(scores - jnp.max(scores, axis=-1, keepdims=True))
    return expo / jnp.sum(expo, axis=-1, keepdims=True)


def hand_over(core, shares, error, mine, send):
    mine[...] = shares[core]
    send[:, :HALF] = shares[1 - core]
    send[:, HALF:] = error


def spatial_kernel(counts, qkv, incoming, gate, mine, send, out):
    tokens, _ = incoming.shape
    member = lax.axis_index("seq")
    live_positions = counts[0, 1]
    keys_live = lax.broadcasted_iota(jnp.int32, (1, tokens), 1) < live_positions

    rows = Shares(out)
    for head in range(HEADS):
        first, last = head_tiles(head)
        keep = head_lanes(head, first, last)
        at = slice(first * LANES, last * LANES)
        queries = jnp.where(keep, qkv[0, :, at], 0)
        scores = dot(queries, qkv[1, :, at], NT) * SCALE
        weights = softmax(jnp.where(keys_live, scores, -1e30)).astype(jnp.bfloat16)
        rows.add(head, first, last, dot(weights, qkv[2, :, at], NN), keep)
    token = lax.broadcasted_iota(jnp.int32, (tokens, 1), 0)
    live = ((token < live_positions) & (member < counts[0, 0])).astype(jnp.float32)
    error = (live * incoming[...].astype(jnp.float32) * gate[...]).astype(jnp.bfloat16)
    hand_over(member % 2, out, error, mine, send)


class Block:
    def __init__(self, counts, arrived):
        self.arrived = arrived
        self.frames, rows, self.width = arrived.shape
        self.positions = rows // 4
        self.tokens = self.frames * self.positions
        query = lax.broadcasted_iota(jnp.int32, (self.tokens, self.tokens), 0)
        key = lax.broadcasted_iota(jnp.int32, (self.tokens, self.tokens), 1)
        same = query % self.positions == key % self.positions
        self.pairs = same & (key // self.positions < counts[0, 0])

    def load(self, which, at=slice(None)):
        block = self.arrived[:, which * self.positions : (which + 1) * self.positions, at]
        return block.reshape(self.tokens, block.shape[-1])

    def weights(self, at, keep):
        scores = dot(jnp.where(keep, self.load(0, at), 0), self.load(1, at), NT) * SCALE
        return softmax(jnp.where(self.pairs, scores, -1e30))


def forward_kernel(counts, arrived, gate, mine, send, out):
    block = Block(counts, arrived)
    member = lax.axis_index("seq")

    rows = Shares(out)
    for head in range(HEADS):
        first, last = head_tiles(head)
        keep = head_lanes(head, first, last)
        at = slice(first * LANES, last * LANES)
        weights = block.weights(at, keep).astype(jnp.bfloat16)
        rows.add(head, first, last, dot(weights, block.load(2, at), NN), keep)
    token = lax.broadcasted_iota(jnp.int32, (block.tokens, 1), 0)
    place = token % block.positions + member * block.positions
    live = (token // block.positions < counts[0, 0]) & (place < counts[0, 1])
    flowing = live.astype(jnp.float32) * block.load(3).astype(jnp.float32)
    hand_over(member % 2, out, (flowing * gate[...]).astype(jnp.bfloat16), mine, send)


def backward_kernel(counts, arrived, send, proj, grads, back):
    block = Block(counts, arrived)
    back[...] = dot(send[:, HALF:], proj[...], NT).astype(jnp.bfloat16)

    def into(which):
        rows = slice(which * block.positions, (which + 1) * block.positions)

        def store(tile, value):
            value = value.reshape(block.frames, block.positions, LANES).astype(jnp.bfloat16)
            grads[:, rows, tile * LANES : (tile + 1) * LANES] = value

        return Rows(store)

    to_q, to_k, to_v = into(0), into(1), into(2)
    for head in range(HEADS):
        first, last = head_tiles(head)
        keep = head_lanes(head, first, last)
        at = slice(first * LANES, last * LANES)
        weights = block.weights(at, keep)
        b = back[:, at]
        to_v.add(head, first, last, dot(weights.astype(jnp.bfloat16), b, TN), keep)
        reaching = dot(jnp.where(keep, b, 0), block.load(2, at), NT)
        reaching = reaching.astype(jnp.bfloat16).astype(jnp.float32)
        drop = jnp.sum(reaching * weights, axis=-1, keepdims=True)
        slope = (weights * (reaching - drop) * SCALE).astype(jnp.bfloat16)
        to_q.add(head, first, last, dot(slope, block.load(1, at), NN), keep)
        to_k.add(head, first, last, dot(slope, block.load(0, at), TN), keep)


def chip_part(mine, send, came):
    return dot(send[:, HALF:], mine[...], TN) + dot(came[:, HALF:], came[:, :HALF], TN)


def part_x_kernel(mine, send, came, part):
    part[...] = chip_part(mine, send, came).astype(jnp.bfloat16).reshape(part.shape)


def part_z_kernel(mine, send, came, part, total, block):
    side = part.shape[0]
    rows = total.shape[0] // side**2
    total[...] = chip_part(mine, send, came)
    for z in range(side):
        for x in range(side):
            start = (x * side + z) * rows
            block[x * rows : (x + 1) * rows, :] = total[start : start + rows, :]
        part[z] = block[...].astype(jnp.bfloat16)


SM = pl.BlockSpec(memory_space=pltpu.SMEM)
VM = pl.BlockSpec(memory_space=pltpu.VMEM)


def shape(*dims):
    return jax.ShapeDtypeStruct(dims, jnp.bfloat16)


def cost(flops):
    return pl.CostEstimate(flops=flops, transcendentals=0, bytes_accessed=4_000_000)


def lines(major):
    side = round(lax.axis_size("dp") ** 0.5)
    if major:
        return [[x * side + z for x in range(side)] for z in range(side)]
    return [[x * side + z for z in range(side)] for x in range(side)]


def near(array):
    return pltpu.with_memory_space_constraint(array, pltpu.VMEM)


def exchange(blocks, axis, groups=None):
    return lax.all_to_all(blocks, axis, split_axis=0, concat_axis=0, tiled=True, axis_index_groups=groups)


def shifts(blocks, axis, here, peers, to):
    came = [lax.dynamic_index_in_dim(blocks, here, 0, keepdims=False)]
    count = lax.axis_size(axis)
    for step in range(1, peers):
        block = lax.dynamic_index_in_dim(blocks, (here + step) % peers, 0, keepdims=False)
        came.append(lax.ppermute(block, axis, [(i, to(i, step)) for i in range(count)]))
    return came


def summed(blocks):
    total = blocks[0].astype(jnp.float32)
    for block in blocks[1:]:
        total = total + block.astype(jnp.float32)
    return total


def part_of(mine, send, z_first):
    width = send.shape[1] - HALF
    side = len(lines(True))
    came = lax.ppermute(send, "seq", [(i, i ^ 1) for i in range(lax.axis_size("seq"))])
    scratch = [pltpu.VMEM((width, HALF), jnp.float32), pltpu.VMEM((width // side, HALF), jnp.float32)]
    return pl.pallas_call(
        part_z_kernel if z_first else part_x_kernel,
        in_specs=[VM] * 3,
        out_specs=VM,
        out_shape=shape(side, width // side, HALF),
        scratch_shapes=scratch if z_first else [],
        cost_estimate=cost(2_000_000_000),
        name="part_z" if z_first else "part_x",
    )(mine, send, came)


def body(spatial_qkv, temporal_qkv, cotangent, spatial_gate, temporal_gate, temporal_proj, live_counts):
    peers = lax.axis_size("seq")
    incoming = cotangent[0, 0]
    tokens, width = incoming.shape
    positions = tokens // peers
    side = len(lines(True))
    x, z = lax.axis_index("dp") // side, lax.axis_index("dp") % side
    along_x = lambda i, n: (i // side + n) % side * side + i % side
    along_z = lambda i, n: i // side * side + (i % side + n) % side
    blocks = jnp.concatenate([temporal_qkv[0, :, 0], cotangent[0]]).reshape(4, peers, positions, width)
    blocks = jnp.moveaxis(blocks, 1, 0).reshape(peers, 4 * positions, width)
    arrived = near(exchange(blocks, "seq"))
    handed = [shape(tokens, HALF), shape(tokens, HALF + width)]
    shares = [pltpu.VMEM((2, tokens, HALF), jnp.bfloat16)]
    mine_s, send_s = pl.pallas_call(
        spatial_kernel,
        in_specs=[SM, VM, VM, VM],
        out_specs=[VM] * 2,
        out_shape=handed,
        scratch_shapes=shares,
        cost_estimate=cost(4_000_000_000),
        name="spatial",
    )(live_counts, near(spatial_qkv[0, :, 0]), near(incoming), spatial_gate)
    came_s = shifts(part_of(mine_s, send_s, True), "dp", z, side, along_z)
    mine_t, send_t = pl.pallas_call(
        forward_kernel,
        in_specs=[SM, VM, VM],
        out_specs=[VM] * 2,
        out_shape=handed,
        scratch_shapes=shares,
        cost_estimate=cost(4_000_000_000),
        name="forward",
    )(live_counts, arrived, temporal_gate)
    part_t = part_of(mine_t, send_t, False)
    came_t = exchange(part_t, "dp", lines(True))
    grads = pl.pallas_call(
        backward_kernel,
        in_specs=[SM, VM, VM, VM],
        out_specs=VM,
        out_shape=shape(peers, 3 * positions, width),
        scratch_shapes=[pltpu.VMEM((tokens, width), jnp.bfloat16)],
        cost_estimate=cost(8_000_000_000),
        name="backward",
    )(live_counts, arrived, send_t, temporal_proj)
    came_t, grads = lax.optimization_barrier((came_t, grads))
    sum_t = summed([came_t[i] for i in range(side)]).astype(jnp.bfloat16)
    came_t = exchange(sum_t.reshape(side, -1, HALF), "dp", lines(False))
    sum_s = summed(came_s).astype(jnp.bfloat16)
    came_t, grads, sum_s = lax.optimization_barrier((came_t, grads, sum_s))
    home = exchange(grads, "seq")
    came_s = shifts(sum_s.reshape(side, -1, HALF), "dp", x, side, along_x)
    both = jnp.stack([summed(came_s), came_t.astype(jnp.float32).sum(axis=0)], axis=1)
    heads = both[:, :, : HEADS // 2 * HD].reshape(-1, 2, HEADS // 2, HD).transpose(2, 1, 0, 3)
    heads = heads.reshape(HEADS // 2, -1, HD)
    home, heads = lax.optimization_barrier((home, heads))
    home = jnp.moveaxis(home.reshape(peers, 3, positions, width), 1, 0).reshape(3, 1, tokens, width)
    chips = [[i for i in range(peers) if i % 2 == c] for c in range(2)]
    rows = exchange(heads, "seq", chips).sum(axis=0).reshape(2, -1, HD)
    return (home[None], rows[0].T, rows[1].T)


def solution(mesh):
    return jax.shard_map(
        body,
        mesh=mesh,
        in_specs=(
            P("dp", None, "seq", None, None),
            P("dp", None, "seq", None, None),
            P("dp", "seq", None, None),
            P("dp", None),
            P("dp", None),
            P(),
            P("dp", None),
        ),
        out_specs=(P("dp", None, "seq", None, None), P("seq", "dp"), P("seq", "dp")),
        check_vma=False,
    )
```

```python
import jax
import jax.numpy as jnp
from jax import lax
from jax.experimental import pallas as pl
from jax.experimental.pallas import tpu as pltpu
from jax.sharding import PartitionSpec as P


HEADS = 16
HD = 72
LANES = 128
HALF = 640
SCALE = HD ** (-0.5)
NN = (((1,), (0,)), ((), ()))
NT = (((1,), (1,)), ((), ()))
TN = (((0,), (0,)), ((), ()))


def dot(left, right, dims):
    return lax.dot_general(left, right, dims, preferred_element_type=jnp.float32)


def head_tiles(head):
    return head * HD // LANES, ((head + 1) * HD + LANES - 1) // LANES


def head_lanes(head, first, last):
    lane = lax.broadcasted_iota(jnp.int32, (1, (last - first) * LANES), 1) + first * LANES
    return (lane >= head * HD) & (lane < (head + 1) * HD)


class Rows:
    def __init__(self, store):
        self.store = store
        self.open = {}

    def add(self, head, first, last, value, keep):
        for tile in range(first, last):
            at = slice((tile - first) * LANES, (tile - first + 1) * LANES)
            piece = value[:, at]
            if tile in self.open:
                piece = jnp.where(keep[:, at], piece, self.open[tile])
            self.open[tile] = piece
        done = (head + 1) * HD // LANES
        for tile in [t for t in self.open if t < done]:
            self.store(tile, self.open.pop(tile))


class Shares:
    def __init__(self, shares):
        self.shares = shares
        self.open = {}

    def add(self, head, first, last, value, keep):
        value = jnp.where(keep, value, 0)
        if last - first == 1:
            value = jnp.concatenate([value, jnp.zeros_like(value)], axis=1)
        core, slot = head % 2, head // 2
        goal = slot * HD // LANES
        shift = (slot * HD - goal * LANES) - (head * HD - first * LANES)
        if shift:
            value = pltpu.roll(value, shift % (2 * LANES), 1)
        for tile in range(goal, ((slot + 1) * HD + LANES - 1) // LANES):
            piece = value[:, (tile - goal) * LANES : (tile - goal + 1) * LANES]
            if (core, tile) in self.open:
                piece = piece + self.open[core, tile]
            self.open[core, tile] = piece
        done = (slot + 1) * HD // LANES if slot + 1 < HEADS // 2 else HALF // LANES
        for key in [k for k in self.open if k[0] == core and k[1] < done]:
            lanes = slice(key[1] * LANES, (key[1] + 1) * LANES)
            self.shares[core, :, lanes] = self.open.pop(key).astype(jnp.bfloat16)


def softmax(scores):
    expo = jnp.exp(scores - jnp.max(scores, axis=-1, keepdims=True))
    return expo / jnp.sum(expo, axis=-1, keepdims=True)


def hand_over(core, shares, error, mine, send):
    mine[...] = shares[core]
    send[:, :HALF] = shares[1 - core]
    send[:, HALF:] = error


def spatial_kernel(counts, qkv, incoming, gate, mine, send, out):
    tokens, _ = incoming.shape
    member = lax.axis_index("seq")
    live_positions = counts[0, 1]
    keys_live = lax.broadcasted_iota(jnp.int32, (1, tokens), 1) < live_positions

    rows = Shares(out)
    for head in range(HEADS):
        first, last = head_tiles(head)
        keep = head_lanes(head, first, last)
        at = slice(first * LANES, last * LANES)
        queries = jnp.where(keep, qkv[0, :, at], 0)
        scores = dot(queries, qkv[1, :, at], NT) * SCALE
        weights = softmax(jnp.where(keys_live, scores, -1e30)).astype(jnp.bfloat16)
        rows.add(head, first, last, dot(weights, qkv[2, :, at], NN), keep)
    token = lax.broadcasted_iota(jnp.int32, (tokens, 1), 0)
    live = ((token < live_positions) & (member < counts[0, 0])).astype(jnp.float32)
    error = (live * incoming[...].astype(jnp.float32) * gate[...]).astype(jnp.bfloat16)
    hand_over(member % 2, out, error, mine, send)


class Block:
    def __init__(self, counts, arrived):
        self.arrived = arrived
        self.frames, rows, self.width = arrived.shape
        self.positions = rows // 4
        self.tokens = self.frames * self.positions
        query = lax.broadcasted_iota(jnp.int32, (self.tokens, self.tokens), 0)
        key = lax.broadcasted_iota(jnp.int32, (self.tokens, self.tokens), 1)
        same = query % self.positions == key % self.positions
        self.pairs = same & (key // self.positions < counts[0, 0])

    def load(self, which, at=slice(None)):
        block = self.arrived[:, which * self.positions : (which + 1) * self.positions, at]
        return block.reshape(self.tokens, block.shape[-1])

    def weights(self, at, keep):
        scores = dot(jnp.where(keep, self.load(0, at), 0), self.load(1, at), NT) * SCALE
        return softmax(jnp.where(self.pairs, scores, -1e30))


def forward_kernel(counts, arrived, gate, mine, send, out):
    block = Block(counts, arrived)
    member = lax.axis_index("seq")

    rows = Shares(out)
    for head in range(HEADS):
        first, last = head_tiles(head)
        keep = head_lanes(head, first, last)
        at = slice(first * LANES, last * LANES)
        weights = block.weights(at, keep).astype(jnp.bfloat16)
        rows.add(head, first, last, dot(weights, block.load(2, at), NN), keep)
    token = lax.broadcasted_iota(jnp.int32, (block.tokens, 1), 0)
    place = token % block.positions + member * block.positions
    live = (token // block.positions < counts[0, 0]) & (place < counts[0, 1])
    flowing = live.astype(jnp.float32) * block.load(3).astype(jnp.float32)
    hand_over(member % 2, out, (flowing * gate[...]).astype(jnp.bfloat16), mine, send)


def backward_kernel(counts, arrived, send, proj, grads, back):
    block = Block(counts, arrived)
    back[...] = dot(send[:, HALF:], proj[...], NT).astype(jnp.bfloat16)

    def into(which):
        rows = slice(which * block.positions, (which + 1) * block.positions)

        def store(tile, value):
            value = value.reshape(block.frames, block.positions, LANES).astype(jnp.bfloat16)
            grads[:, rows, tile * LANES : (tile + 1) * LANES] = value

        return Rows(store)

    to_q, to_k, to_v = into(0), into(1), into(2)
    for head in range(HEADS):
        first, last = head_tiles(head)
        keep = head_lanes(head, first, last)
        at = slice(first * LANES, last * LANES)
        weights = block.weights(at, keep)
        b = back[:, at]
        to_v.add(head, first, last, dot(weights.astype(jnp.bfloat16), b, TN), keep)
        reaching = dot(jnp.where(keep, b, 0), block.load(2, at), NT)
        reaching = reaching.astype(jnp.bfloat16).astype(jnp.float32)
        drop = jnp.sum(reaching * weights, axis=-1, keepdims=True)
        slope = (weights * (reaching - drop) * SCALE).astype(jnp.bfloat16)
        to_q.add(head, first, last, dot(slope, block.load(1, at), NN), keep)
        to_k.add(head, first, last, dot(slope, block.load(0, at), TN), keep)


def part_kernel(mine, send, came, part):
    total = dot(send[:, HALF:], mine[...], TN) + dot(came[:, HALF:], came[:, :HALF], TN)
    part[...] = total.astype(jnp.bfloat16).reshape(part.shape)


SM = pl.BlockSpec(memory_space=pltpu.SMEM)
VM = pl.BlockSpec(memory_space=pltpu.VMEM)


def shape(*dims):
    return jax.ShapeDtypeStruct(dims, jnp.bfloat16)


def cost(flops):
    return pl.CostEstimate(flops=flops, transcendentals=0, bytes_accessed=4_000_000)


def lines(major):
    side = round(lax.axis_size("dp") ** 0.5)
    if major:
        return [[x * side + z for x in range(side)] for z in range(side)]
    return [[x * side + z for z in range(side)] for x in range(side)]


def near(array):
    return pltpu.with_memory_space_constraint(array, pltpu.VMEM)


def exchange(blocks, axis, groups=None):
    return lax.all_to_all(blocks, axis, split_axis=0, concat_axis=0, tiled=True, axis_index_groups=groups)


def shifts(blocks, axis, here, peers, to):
    came = [lax.dynamic_index_in_dim(blocks, here, 0, keepdims=False)]
    count = lax.axis_size(axis)
    for step in range(1, peers):
        block = lax.dynamic_index_in_dim(blocks, (here + step) % peers, 0, keepdims=False)
        came.append(lax.ppermute(block, axis, [(i, to(i, step)) for i in range(count)]))
    return came


def summed(blocks):
    total = blocks[0].astype(jnp.float32)
    for block in blocks[1:]:
        total = total + block.astype(jnp.float32)
    return total


def part_of(mine, send):
    width = send.shape[1] - HALF
    side = len(lines(True))
    came = lax.ppermute(send, "seq", [(i, i ^ 1) for i in range(lax.axis_size("seq"))])
    return pl.pallas_call(
        part_kernel,
        in_specs=[VM] * 3,
        out_specs=VM,
        out_shape=shape(side, width // side, HALF),
        cost_estimate=cost(2_000_000_000),
        name="part",
    )(mine, send, came)


def body(spatial_qkv, temporal_qkv, cotangent, spatial_gate, temporal_gate, temporal_proj, live_counts):
    peers = lax.axis_size("seq")
    incoming = cotangent[0, 0]
    tokens, width = incoming.shape
    positions = tokens // peers
    side = len(lines(True))
    z = lax.axis_index("dp") % side
    along_z = lambda i, n: i // side * side + (i % side + n) % side
    blocks = jnp.concatenate([temporal_qkv[0, :, 0], cotangent[0]]).reshape(4, peers, positions, width)
    blocks = jnp.moveaxis(blocks, 1, 0).reshape(peers, 4 * positions, width)
    arrived = near(exchange(blocks, "seq"))
    handed = [shape(tokens, HALF), shape(tokens, HALF + width)]
    shares = [pltpu.VMEM((2, tokens, HALF), jnp.bfloat16)]
    mine_s, send_s = pl.pallas_call(
        spatial_kernel,
        in_specs=[SM, VM, VM, VM],
        out_specs=[VM] * 2,
        out_shape=handed,
        scratch_shapes=shares,
        cost_estimate=cost(4_000_000_000),
        name="spatial",
    )(live_counts, near(spatial_qkv[0, :, 0]), near(incoming), spatial_gate)
    part_s = part_of(mine_s, send_s)
    arrived, _ = lax.optimization_barrier((arrived, part_s))
    sum_s = lax.psum_scatter(part_s, "dp", scatter_dimension=0, tiled=True, axis_index_groups=lines(True))[0]
    mine_t, send_t = pl.pallas_call(
        forward_kernel,
        in_specs=[SM, VM, VM],
        out_specs=[VM] * 2,
        out_shape=handed,
        scratch_shapes=shares,
        cost_estimate=cost(4_000_000_000),
        name="forward",
    )(live_counts, arrived, temporal_gate)
    part_t = part_of(mine_t, send_t)
    came_t = exchange(part_t, "dp", lines(True))
    grads = pl.pallas_call(
        backward_kernel,
        in_specs=[SM, VM, VM, VM],
        out_specs=VM,
        out_shape=shape(peers, 3 * positions, width),
        scratch_shapes=[pltpu.VMEM((tokens, width), jnp.bfloat16)],
        cost_estimate=cost(8_000_000_000),
        name="backward",
    )(live_counts, arrived, send_t, temporal_proj)
    came_t, grads = lax.optimization_barrier((came_t, grads))
    home = exchange(grads, "seq")
    sum_t = summed([came_t[i] for i in range(side)])
    sums = jnp.concatenate([sum_s, sum_t.astype(jnp.bfloat16)], axis=1)
    came = shifts(sums.reshape(side, -1, 2 * HALF), "dp", z, side, along_z)
    both = summed(came).reshape(-1, 2, HALF)
    heads = both[:, :, : HEADS // 2 * HD].reshape(-1, 2, HEADS // 2, HD).transpose(2, 1, 0, 3)
    heads = heads.reshape(HEADS // 2, -1, HD)
    home, heads = lax.optimization_barrier((home, heads))
    home = jnp.moveaxis(home.reshape(peers, 3, positions, width), 1, 0).reshape(3, 1, tokens, width)
    chips = [[i for i in range(peers) if i % 2 == c] for c in range(2)]
    rows = exchange(heads, "seq", chips).sum(axis=0).reshape(2, -1, HD)
    return (home[None], rows[0].T, rows[1].T)


def solution(mesh):
    return jax.shard_map(
        body,
        mesh=mesh,
        in_specs=(
            P("dp", None, "seq", None, None),
            P("dp", None, "seq", None, None),
            P("dp", "seq", None, None),
            P("dp", None),
            P("dp", None),
            P(),
            P("dp", None),
        ),
        out_specs=(P("dp", None, "seq", None, None), P("seq", "dp"), P("seq", "dp")),
        check_vma=False,
    )
```
